128 devices in a mesh: section: 4 (over y), wide: 8 (over z, x_hi), narrow: 4 (over x_lo, core).
Axes of the slice: x: 4 (x_hi: 2, x_lo: 2; x = x_hi * 2 + x_lo), y: 4, z: 4, core: 2. Of those that a mesh axis runs over, the one named last changes fastest.
Arguments:
- normed_inputs: bfloat16 [4, 4, 4, 768, 4096], P('section', 'narrow', None, 'wide'), may hold values from -160 to 160
- value_cotangent: bfloat16 [4, 4, 4, 768, 1024], P('section', 'narrow', None, 'wide'), may hold values from -6 to 6
- expert_hidden: bfloat16 [4, 4, 4, 256, 7168], P('section', 'narrow', None, None, 'wide'), may hold values from -40 to 40
- expert_cotangent: bfloat16 [4, 4, 4, 256, 4096], P('section', 'narrow', None, 'wide'), may hold values from -110 to 110
- slot_gate: bfloat16 [4, 4, 4, 256], P('section', 'narrow', None, 'wide'), may hold values from 0.25 to 1
- slot_count: int32 [4, 4, 4], P('section', 'narrow'), may hold values from 129 to 256, as said below
- expert_weight: bfloat16 [4, 7168, 4096], P('section', 'wide', 'narrow'), may hold values from -0.0625 to 0.0625
- expert_moment: float32 [4, 7168, 4096], P('section', 'wide', 'narrow'), may hold values from -6 to 6
- value_weight: bfloat16 [4, 4096, 1024], P('section', ('wide', 'narrow')), may hold values from -0.09375 to 0.09375
- value_moment: float32 [4, 4096, 1024], P('section', ('wide', 'narrow')), may hold values from -6 to 6
Outputs:
- expert_weight_next: bfloat16 [4, 7168, 4096], P('section', 'wide', 'narrow')
- expert_moment_next: float32 [4, 7168, 4096], P('section', 'wide', 'narrow')
- value_weight_next: bfloat16 [4, 4096, 1024], P('section', ('wide', 'narrow'))
- value_moment_next: float32 [4, 4096, 1024], P('section', ('wide', 'narrow'))
The draws below stay inside these ranges and needn't reach their ends.
Inputs may be any that keep to these rules, and one draw needn't show every extreme that they name: The live slots of a micro-batch are slots 0 to slot_count - 1; in every layer and replica some micro-batch fills all 256 slots.
All inputs are finite; a program needn't handle non-finite values.
Results may differ from the reference program's by a relative error of at most 0.014.
Values may be sent and summed in bfloat16 or wider, within the bound.
No kernel may reach another device: no remote copies, remote signals or barrier semaphores. Data moves between devices by JAX's collectives and lax.ppermute only.
A program may use at most 128 MiB of HBM per device.

```python
import math
import jax
import jax.numpy as jnp
from jax import lax

D = 4096
FF = 7168
KV = 1024
MICRO = 4
MB_DEV = 96
SECTIONS = 4
REPLICAS = 4
SEQ = 768
SLOTS = 256
N_WIDE = 8


def rough_field(base_key, extent, section_rise, divisor):
    subkeys = jax.random.split(base_key, 3)
    columns = extent[-1]
    layers = extent[0]
    column_pos = jnp.arange(columns, dtype=jnp.float32) / max(columns - 1, 1)
    column_scale = jnp.exp(math.log(3.0) * column_pos + jax.random.uniform(subkeys[0], (columns,), jnp.float32, 0.0, math.log(3.3)))
    layer_pos = jnp.arange(layers, dtype=jnp.float32) / max(layers - 1, 1)
    layer_scale = jnp.exp(section_rise * math.log(3.0) * layer_pos).reshape(layers, 1, 1, 1, 1)
    row_scale = jnp.exp(jax.random.uniform(subkeys[1], extent[:-1] + (1,), jnp.float32, 0.0, math.log(3.0)))
    values = jnp.clip(jax.random.normal(subkeys[2], extent, jnp.float32), -6.0, 6.0)
    return values * row_scale * column_scale * layer_scale / divisor


def draw_normed_inputs(key, part):
    return rough_field(jax.random.fold_in(key, 3), (SECTIONS, REPLICAS, MICRO, SEQ, D), 1.0, 4.0).astype(jnp.bfloat16)


def draw_expert_hidden(key, part):
    return rough_field(jax.random.fold_in(key, 5), (SECTIONS, REPLICAS, MICRO, SLOTS, FF), 0.0, 6.0).astype(jnp.bfloat16)


def draw_expert_cotangent(key, part):
    return rough_field(jax.random.fold_in(key, 7), (SECTIONS, REPLICAS, MICRO, SLOTS, D), 1.0, 6.0).astype(jnp.bfloat16)


def draw_slot_count(key, part):
    count_key = jax.random.fold_in(key, 11)
    pick_key = jax.random.fold_in(key, 13)
    counts = jax.random.randint(count_key, (SECTIONS, REPLICAS, MICRO), SLOTS // 2 + 1, SLOTS + 1, dtype=jnp.int32)
    chosen = jax.random.randint(pick_key, (SECTIONS, REPLICAS, 1), 0, MICRO, dtype=jnp.int32)
    positions = jnp.arange(MICRO, dtype=jnp.int32).reshape(1, 1, MICRO)
    return jnp.where(positions == chosen, jnp.int32(SLOTS), counts).astype(jnp.int32)


def block_scale(key, dims, cuts, smallest, high):
    level = 1.0
    for position, parts in cuts:
        heights = jax.random.uniform(jax.random.fold_in(jax.random.fold_in(key, 6), position), (parts,), jnp.float32, smallest / len(cuts), high / len(cuts))
        level = level * jnp.repeat(jnp.exp(heights), dims[position] // parts).reshape((-1,) + (1,) * (len(dims) - 1 - position))
    return level


def scatter_about(key, shape, deviation, reach, shards=(), held_as=jnp.bfloat16):
    level = block_scale(key, shape, shards, -0.22, 0.18) if shards else 1.0
    entries = jax.random.normal(key, shape, jnp.float32) * deviation * level
    return jnp.minimum(jnp.maximum(entries, -reach), reach).astype(held_as)


def setup_inputs(seed: int = 0) -> dict:
    key_of = jax.random.split(jax.random.key(seed), 11)
    normed_inputs = draw_normed_inputs(jax.random.fold_in(key_of[10], 71), 0)
    value_cotangent = scatter_about(key_of[1], (SECTIONS, REPLICAS, MICRO, SEQ, KV), 1.0, 6.0, ((0, 4), (1, 4), (3, 8)))
    expert_hidden = draw_expert_hidden(jax.random.fold_in(key_of[10], 71), 0)
    expert_cotangent = draw_expert_cotangent(jax.random.fold_in(key_of[10], 71), 0)
    slot_gate = jnp.clip(0.25 + 0.75 * jax.random.uniform(key_of[4], (SECTIONS, REPLICAS, MICRO, SLOTS), jnp.float32) ** block_scale(key_of[4], (SECTIONS, REPLICAS, MICRO, SLOTS), ((0, 4), (1, 4), (3, 8)), -0.2, 0.2), 0.25, 1.0).astype(jnp.bfloat16)
    slot_count = draw_slot_count(jax.random.fold_in(key_of[10], 71), 0)
    expert_weight = scatter_about(key_of[6], (SECTIONS, FF, D), FF ** -0.5, 0.0625, ((0, 4), (1, 8), (2, 4)))
    expert_moment = scatter_about(key_of[7], (SECTIONS, FF, D), 1.0, 6.0, ((0, 4), (1, 8), (2, 4)), jnp.float32)
    value_weight = scatter_about(key_of[8], (SECTIONS, D, KV), D ** -0.5, 0.09375, ((0, 4), (1, 32)))
    value_moment = scatter_about(key_of[9], (SECTIONS, D, KV), 1.0, 6.0, ((0, 4), (1, 32)), jnp.float32)
    return {"normed_inputs": normed_inputs, "value_cotangent": value_cotangent, "expert_hidden": expert_hidden, "expert_cotangent": expert_cotangent, "slot_gate": slot_gate, "slot_count": slot_count, "expert_weight": expert_weight, "expert_moment": expert_moment, "value_weight": value_weight, "value_moment": value_moment}


MOMENTUM_DECAY = 0.9
STEP_RATE = 0.01

def rounded_add(accumulated, product):
    kept = lax.optimization_barrier(product.astype(jnp.bfloat16))
    return accumulated + kept.astype(jnp.float32)

def expert_layer(hidden_layer, cotangent_layer, gate_layer, count_layer):
    positions = jnp.arange(SLOTS, dtype=jnp.int32)
    live = positions[None, None, :] < count_layer[:, :, None]
    coefficient = jnp.where(live, gate_layer.astype(jnp.float32), jnp.zeros(gate_layer.shape, jnp.float32))
    scaled = (coefficient[..., None] * cotangent_layer.astype(jnp.float32)).astype(jnp.bfloat16)

    def add_replica(accumulated, pieces):
        hidden_rows = pieces[0].reshape(-1, FF)
        scaled_rows = pieces[1].reshape(-1, D)
        product = jnp.dot(hidden_rows.T, scaled_rows, preferred_element_type=jnp.float32)
        return (rounded_add(accumulated, product), None)
    result, ignored = lax.scan(add_replica, jnp.zeros((FF, D), jnp.float32), (hidden_layer, scaled))
    return result

def value_layer(input_layer, cotangent_layer):
    device_inputs = input_layer.reshape(REPLICAS, MICRO, N_WIDE, MB_DEV, D).transpose(0, 2, 1, 3, 4).reshape(REPLICAS * N_WIDE, MICRO * MB_DEV, D)
    device_cotangents = cotangent_layer.reshape(REPLICAS, MICRO, N_WIDE, MB_DEV, KV).transpose(0, 2, 1, 3, 4).reshape(REPLICAS * N_WIDE, MICRO * MB_DEV, KV)

    def add_device(accumulated, pieces):
        product = jnp.dot(pieces[0].T, pieces[1], preferred_element_type=jnp.float32)
        return (rounded_add(accumulated, product), None)
    result, ignored = lax.scan(add_device, jnp.zeros((D, KV), jnp.float32), (device_inputs, device_cotangents))
    return result

def reference(normed_inputs, value_cotangent, expert_hidden, expert_cotangent, slot_gate, slot_count, expert_weight, expert_moment, value_weight, value_moment):
    expert_grads = []
    value_grads = []
    for layer_index in range(SECTIONS):
        expert_grads.append(expert_layer(expert_hidden[layer_index], expert_cotangent[layer_index], slot_gate[layer_index], slot_count[layer_index]))
        value_grads.append(value_layer(normed_inputs[layer_index], value_cotangent[layer_index]))
    expert_grad = jnp.stack(expert_grads)
    value_grad = jnp.stack(value_grads)
    overall = jnp.sum(expert_grad * expert_grad) + jnp.sum(value_grad * value_grad)
    entry_count = SECTIONS * (FF * D + D * KV)
    factor = jnp.minimum(1.0, math.sqrt(entry_count) / jnp.sqrt(overall + 1e-06))
    expert_next = MOMENTUM_DECAY * expert_moment + factor * expert_grad
    value_next = MOMENTUM_DECAY * value_moment + factor * value_grad
    expert_weight_next = (expert_weight.astype(jnp.float32) - STEP_RATE * expert_next).astype(jnp.bfloat16)
    value_weight_next = (value_weight.astype(jnp.float32) - STEP_RATE * value_next).astype(jnp.bfloat16)
    return (expert_weight_next, expert_next, value_weight_next, value_next)
```

```python
import math

import jax
import jax.numpy as jnp
from jax import lax
from jax.sharding import Mesh
from jax.sharding import PartitionSpec as P

D = 4096
FF = 7168
KV = 1024
WIDE = ("z", "xh")
NARROW = ("xl", "c")
ROW = ("xh", "xl", "c")
X = ("xh", "xl")
WIDE_NARROW = ("z", "xh", "xl", "c")

MOMENTUM_DECAY = 0.9
STEP_RATE = 0.01
Z_FIRST = 512


def flip(value, axes, size, bits):
    return lax.ppermute(value, axes, [(i, i ^ bits) for i in range(size)])


def shift(value, axes, step):
    return lax.ppermute(value, axes, [(i, (i + step) % 4) for i in range(4)])


def pick(array, index, dim):
    return lax.dynamic_index_in_dim(array, index, dim, keepdims=False)


def wide_sum(*terms):
    total = terms[0].astype(jnp.float32)
    for term in terms[1:]:
        total = total + term.astype(jnp.float32)
    return total


def ring_scatter(blocks, axes, place, dim):
    opposite = pick(blocks, (place + 2) % 4, dim)
    half = opposite.shape[0] // 2
    from_low = shift(opposite[:half], axes, 1)
    from_high = shift(opposite[half:], axes, -1)
    onward = pick(blocks, (place + 1) % 4, dim)
    back = pick(blocks, (place + 3) % 4, dim)
    onward = jnp.concatenate(
        [wide_sum(onward[:half], from_low).astype(jnp.bfloat16), onward[half:]]
    )
    back = jnp.concatenate([back[:half], wide_sum(back[half:], from_high).astype(jnp.bfloat16)])
    return wide_sum(pick(blocks, place, dim), shift(onward, axes, 1), shift(back, axes, -1))


def on_device(
    normed_inputs,
    value_cotangent,
    expert_hidden,
    expert_cotangent,
    slot_gate,
    slot_count,
    expert_weight,
    expert_moment,
    value_weight,
    value_moment,
):
    z = lax.axis_index("z")
    xh = lax.axis_index("xh")
    xl = lax.axis_index("xl")
    c = lax.axis_index("c")
    x = xh * 2 + xl

    positions = (z * 2 + xh) * 32 + jnp.arange(32, dtype=jnp.int32)
    live = positions[None, :] < slot_count[0, 0][:, None]
    gate = slot_gate[0, 0].astype(jnp.float32)
    coefficient = jnp.where(live, gate, jnp.zeros(gate.shape, jnp.float32))
    cotangent = expert_cotangent[0, 0]
    scaled = []
    for bits in range(4):
        block = (xl * 2 + c) ^ bits
        piece = lax.dynamic_slice_in_dim(cotangent, block * 1024, 1024, 2)
        piece = (coefficient[:, :, None] * piece.astype(jnp.float32)).astype(jnp.bfloat16)
        scaled.append(piece.reshape(128, 1024))
    rows = {}
    for bits in (4, 5, 6, 7, 2, 3, 1):
        rows[bits] = flip(scaled[bits % 4], ROW, 8, bits)
    rows[0] = scaled[0]
    own_low = jnp.concatenate([rows[0], rows[4], rows[1], rows[5]])
    own_high = jnp.concatenate([rows[2], rows[6], rows[3], rows[7]])

    inputs = normed_inputs[0, 0].reshape(384, 16, 2, 128)
    inputs_own = pick(inputs, c, 2).reshape(384, 2048)
    inputs_peer = flip(pick(inputs, 1 - c, 2).reshape(384, 2048), "c", 2, 1)
    tokens_own = value_cotangent[0, 0].reshape(384, KV)
    tokens_peer = flip(tokens_own, "c", 2, 1)
    value_part = lax.dot_general(
        jnp.concatenate([inputs_own, inputs_peer]),
        jnp.concatenate([tokens_own, tokens_peer]),
        (((0,), (0,)), ((), ())),
        preferred_element_type=jnp.float32,
    ).astype(jnp.bfloat16)
    value_part = value_part.reshape(4, 4, 128, KV)

    hidden = expert_hidden[0, 0]
    order = [z, (z + 3) % 4, (z + 1) % 4, (z + 2) % 4]
    hidden_rows = []
    for source in order:
        for bits in range(2):
            start = (source * 2 + (xh ^ bits)) * 32
            hidden_rows.append(lax.dynamic_slice_in_dim(hidden, start, 32, 1).reshape(128, 896))
    hidden_most = [jnp.concatenate(hidden_rows[:6])]
    hidden_last = [jnp.concatenate(hidden_rows[6:])]
    for held in (hidden_most, hidden_last):
        held.append(flip(held[0], "c", 2, 1))
        held.append(flip(held[0], X, 4, 1))
        held.append(flip(held[2], "c", 2, 1))

    low_up = shift(own_low, "z", 1)
    high_down = shift(own_high, "z", -1)
    high_up = shift(own_high, "z", 1)
    low_down = shift(own_low, "z", -1)
    low_far = shift(low_up, "z", 1)
    high_far = shift(high_down, "z", -1)

    value_z = ring_scatter(
        value_part[..., :Z_FIRST].reshape(4, 512, Z_FIRST), "z", z, 0
    ).astype(jnp.bfloat16)
    value_z = ring_scatter(value_z.reshape(4, 128, Z_FIRST), X, x, 0)
    rest = KV - Z_FIRST
    value_x = ring_scatter(value_part[..., Z_FIRST:], X, x, 1).astype(jnp.bfloat16)
    value_x = ring_scatter(value_x, "z", z, 0)
    value_grad = jnp.concatenate([value_z, value_x], axis=1)

    def contract(held, lows, highs):
        count = len(lows)
        left = jnp.concatenate(
            [held[r][k * 256 : k * 256 + 256] for k in range(count) for r in range(4)]
        )
        right = jnp.concatenate([p for k in range(count) for p in (lows[k], highs[k])])
        return lax.dot_general(
            left, right, (((0,), (0,)), ((), ())), preferred_element_type=jnp.float32
        )

    expert_grad = contract(hidden_most, [own_low, low_up, low_down], [own_high, high_up, high_down])
    expert_grad = expert_grad + contract(hidden_last, [low_far], [high_far])

    squares = jnp.sum(expert_grad * expert_grad) + jnp.sum(value_grad * value_grad)
    slot = jnp.broadcast_to(squares, (1, 128))
    slot = slot + flip(slot, "c", 2, 1)
    spread = jnp.broadcast_to(slot[None], (64, 1, 128))
    spread = lax.all_to_all(spread, ("section", "z", "xh", "xl"), 0, 0, tiled=True)
    overall = jnp.sum(spread[:, 0, 0])
    entry_count = lax.axis_size("section") * (FF * D + D * KV)
    factor = jnp.minimum(1.0, math.sqrt(entry_count) / jnp.sqrt(overall + 1e-06))
    expert_next = MOMENTUM_DECAY * expert_moment[0] + factor * expert_grad
    value_next = MOMENTUM_DECAY * value_moment[0] + factor * value_grad
    expert_weight_next = (expert_weight[0].astype(jnp.float32) - STEP_RATE * expert_next).astype(
        jnp.bfloat16
    )
    value_weight_next = (value_weight[0].astype(jnp.float32) - STEP_RATE * value_next).astype(
        jnp.bfloat16
    )
    return (expert_weight_next[None], expert_next[None], value_weight_next[None], value_next[None])


def solution(mesh):
    finer = Mesh(
        mesh.devices.reshape(mesh.shape["section"], 4, 2, 2, 2),
        ("section", "z", "xh", "xl", "c"),
    )
    in_specs = (
        P("section", NARROW, None, WIDE, None),
        P("section", NARROW, None, WIDE, None),
        P("section", NARROW, None, None, WIDE),
        P("section", NARROW, None, WIDE, None),
        P("section", NARROW, None, WIDE),
        P("section", NARROW, None),
        P("section", WIDE, NARROW),
        P("section", WIDE, NARROW),
        P("section", WIDE_NARROW, None),
        P("section", WIDE_NARROW, None),
    )
    out_specs = (
        P("section", WIDE, NARROW),
        P("section", WIDE, NARROW),
        P("section", WIDE_NARROW, None),
        P("section", WIDE_NARROW, None),
    )
    return jax.shard_map(
        on_device, mesh=finer, in_specs=in_specs, out_specs=out_specs, check_vma=False
    )
```

```python
import math

import jax
import jax.numpy as jnp
from jax import lax
from jax.experimental import pallas as pl
from jax.experimental.pallas import tpu as pltpu
from jax.sharding import Mesh
from jax.sharding import PartitionSpec as P

D = 4096
FF = 7168
KV = 1024
WIDE = ("z", "xh")
NARROW = ("xl", "c")
ROW = ("xh", "xl", "c")
X = ("xh", "xl")
WIDE_NARROW = ("z", "xh", "xl", "c")

MOMENTUM_DECAY = 0.9
STEP_RATE = 0.01


def flip(value, axes, size, bits):
    return lax.ppermute(value, axes, [(i, i ^ bits) for i in range(size)])


def shift(value, axes, step):
    return lax.ppermute(value, axes, [(i, (i + step) % 4) for i in range(4)])


def wide_sum(*terms):
    total = terms[0].astype(jnp.float32)
    for term in terms[1:]:
        total = total + term.astype(jnp.float32)
    return total


F32 = jnp.float32
BF16 = jnp.bfloat16


def like(*shape, dtype=BF16):
    return jax.ShapeDtypeStruct(shape, dtype)


def params(mebibytes):
    return pltpu.CompilerParams(vmem_limit_bytes=mebibytes << 20)


SMEM = pl.BlockSpec(memory_space=pltpu.SMEM)
VMEM = pl.BlockSpec(memory_space=pltpu.VMEM)


def scale_body(place, count, gate, cotangent, *outs):
    eye = lax.broadcasted_iota(jnp.int32, (32, 32), 0) == lax.broadcasted_iota(
        jnp.int32, (32, 32), 1
    )
    position = (place[0] * 2 + place[1]) * 32 + lax.broadcasted_iota(jnp.int32, (32, 1), 0)
    for m in range(4):
        row = gate[0, 0, m : m + 1, :].astype(F32)
        column = jnp.sum(jnp.where(eye, row, 0.0), axis=1, keepdims=True)
        coefficient = jnp.where(position < count[0, 0, m], column, 0.0)
        for bits in range(4):
            start = pl.multiple_of(((place[2] * 2 + place[3]) ^ bits) * 1024, 1024)
            piece = cotangent[0, 0, m, :, pl.ds(start, 1024)].astype(F32)
            outs[bits][m * 32 : m * 32 + 32, :] = (coefficient * piece).astype(BF16)


def scale(place, count, gate, cotangent):
    return pl.pallas_call(
        scale_body,
        in_specs=[SMEM, SMEM, VMEM, VMEM],
        out_specs=[VMEM] * 4,
        out_shape=[like(128, 1024)] * 4,
        compiler_params=params(8),
        name="scale",
    )(place, count, gate, cotangent)


def hidden_body(place, hidden, first, second):
    turned = hidden[0, 0].reshape(128, 896).T
    step = pl.program_id(0)

    @pl.when(step < 4)
    def _():
        first[...] = turned

    @pl.when(step >= 4)
    def _():
        second[...] = turned


def hidden_source(i, place):
    chunk = i // 2
    offset = jnp.where(chunk == 1, 3, jnp.where(chunk == 2, 1, jnp.where(chunk == 3, 2, 0)))
    source = (place[0] + offset) % 4
    return (0, 0, 0, source * 2 + (place[1] ^ (i % 2)), 0)


def arrange_hidden(place, hidden):
    return pl.pallas_call(
        hidden_body,
        grid_spec=pltpu.PrefetchScalarGridSpec(
            num_scalar_prefetch=1,
            grid=(8,),
            in_specs=[pl.BlockSpec((1, 1, 4, 32, 896), hidden_source)],
            out_specs=[
                pl.BlockSpec((896, 128), lambda i, place: (0, jnp.minimum(i, 3))),
                pl.BlockSpec((896, 128), lambda i, place: (0, jnp.maximum(i, 4) - 4)),
            ],
        ),
        out_shape=[like(896, 512)] * 2,
        compiler_params=params(6),
        name="arrange_hidden",
    )(place, hidden)


def value_body(place, left_own, left_peer, right_own, right_peer, *refs):
    outs, turned = refs[:4], refs[4]

    @pl.when(pl.program_id(0) == 0)
    def _():
        half = pl.ds(pl.multiple_of(place[3] * 512, 512), 512)
        turned[:, :384] = right_own[0, 0, :, :, half].reshape(384, 512).T
        turned[:, 384:] = right_peer[0, 0, :, :, half].reshape(384, 512).T

    for bits in range(4):
        x = (place[1] * 2 + place[2]) ^ bits
        columns = pl.ds(pl.multiple_of(x * 256, 256), 256)
        left = jnp.concatenate(
            [ref[0, 0, :, :, columns].reshape(384, 256) for ref in (left_own, left_peer)]
        )
        outs[bits][0] = jnp.dot(turned[...], left, preferred_element_type=F32).astype(BF16)


def value_product(place, left_own, left_peer, right_own, right_peer):
    left = pl.BlockSpec((1, 1, 4, 96, 1024), lambda i, place: (0, 0, 0, 0, i))
    right = pl.BlockSpec((1, 1, 4, 96, KV), lambda i, place: (0, 0, 0, 0, 0))
    return pl.pallas_call(
        value_body,
        grid_spec=pltpu.PrefetchScalarGridSpec(
            num_scalar_prefetch=1,
            grid=(4,),
            in_specs=[left, left, right, right],
            out_specs=[pl.BlockSpec((1, 512, 256), lambda i, place: (i, 0, 0))] * 4,
            scratch_shapes=[pltpu.VMEM((512, 768), BF16)],
        ),
        out_shape=[like(4, 512, 256)] * 4,
        compiler_params=params(20),
        cost_estimate=pl.CostEstimate(
            flops=3221225472, bytes_accessed=12000000, transcendentals=0
        ),
        name="value_product",
    )(place, left_own, left_peer, right_own, right_peer)


def spread_body(place, own, first, second, *outs):
    total = own[0].astype(F32) + first[0].astype(F32) + second[0].astype(F32)
    for bits in range(4):

        @pl.when(pl.program_id(0) == bits)
        def _():
            outs[bits][...] = total.astype(BF16)


def spread_rows(place, own, first, second):
    block = pl.BlockSpec((1, 512, 256), lambda i, place: (place[0] ^ i, 0, 0))
    return pl.pallas_call(
        spread_body,
        grid_spec=pltpu.PrefetchScalarGridSpec(
            num_scalar_prefetch=1,
            grid=(4,),
            in_specs=[block] * 3,
            out_specs=[pl.BlockSpec((512, 256), lambda i, place: (0, 0))] * 4,
        ),
        out_shape=[like(512, 256)] * 4,
        compiler_params=params(8),
        name="spread_rows",
    )(place, own, first, second)


def halve_body(place, *refs):
    terms, (mine, other, total) = refs[:4], refs[4:]
    total[...] = sum(term[...].astype(F32) for term in terms)
    mine[...] = total[:, pl.ds(pl.multiple_of(place[3] * 128, 128), 128)]
    other[...] = total[:, pl.ds(pl.multiple_of(128 - place[3] * 128, 128), 128)]


def halve(place, *terms):
    return pl.pallas_call(
        halve_body,
        in_specs=[SMEM] + [VMEM] * 4,
        out_specs=[VMEM] * 2,
        out_shape=[like(512, 128, dtype=F32)] * 2,
        scratch_shapes=[pltpu.VMEM((512, 256), F32)],
        compiler_params=params(6),
        name="halve",
    )(place, *terms)


def stack_body(*refs):
    for n, ref in enumerate(refs[:-1]):
        refs[-1][n * 128 : n * 128 + 128, :] = ref[...]


def stack(*pieces):
    return pl.pallas_call(
        stack_body,
        in_specs=[VMEM] * len(pieces),
        out_specs=VMEM,
        out_shape=like(128 * len(pieces), 1024),
        compiler_params=params(6),
        name="stack",
    )(*pieces)


def contract(hidden, places, rows, start=None, value=None):
    count = len(places)
    width = 256

    def body(*refs):
        held = refs[: 4 * count]
        pieces = refs[4 * count : 7 * count]
        rest = list(refs[7 * count :])
        columns = pl.ds(pl.multiple_of(pl.program_id(0) * width, width), width)
        left = jnp.concatenate([h[...] for h in held], axis=1)
        right = []
        for n in range(count):
            near, high, far = pieces[3 * n : 3 * n + 3]
            right += [near[:128], far[:128], near[128:], far[128:], high[...]]
        total = jnp.dot(left, jnp.concatenate(right), preferred_element_type=F32)
        if start is not None:
            total = total + rest.pop(0)[:, columns]
        if value is not None:
            mine, other = rest.pop(0), rest.pop(0)
        rest[0][:, columns] = total
        if value is not None:
            slot = rest[1]
            folded = jnp.sum((total * total).reshape(112, 8, width), axis=0)
            folded = folded[:, :128] + folded[:, 128:]

            @pl.when(pl.program_id(0) == 0)
            def _():
                own = mine[...] * mine[...] + other[...] * other[...]
                slot[:8, :] = folded + jnp.sum(own.reshape(64, 8, 128), axis=0)

            @pl.when(pl.program_id(0) > 0)
            def _():
                slot[:8, :] = slot[:8, :] + folded

            @pl.when(pl.program_id(0) == 3)
            def _():
                slot[...] = jnp.broadcast_to(
                    jnp.sum(slot[:8, :], axis=0, keepdims=True), (128, 128)
                )

    def held(k):
        return pl.BlockSpec((896, 256), lambda i: (0, k))

    def piece(rows):
        return pl.BlockSpec((rows, width), lambda i: (0, i))

    extra = [] if start is None else [start]
    extra += [] if value is None else list(value)
    out_shape = [pltpu.VMEM((896, 1024), F32)]
    if value is not None:
        out_shape.append(like(128, 128, dtype=F32))
    return pl.pallas_call(
        body,
        grid=(1024 // width,),
        in_specs=[held(k) for k in places for _ in range(4)]
        + [piece(256), piece(512), piece(256)] * count
        + [VMEM] * len(extra),
        out_specs=[VMEM] * len(out_shape),
        out_shape=out_shape,
        cost_estimate=pl.CostEstimate(
            flops=count * 1879048192, bytes_accessed=count * 4000000, transcendentals=0
        ),
        compiler_params=params(28),
        name="contract",
    )(*[h for _ in places for h in hidden], *[p for three in rows for p in three], *extra)


def load_body(moment, weight, moment_out, weight_out, sems):
    copies = [
        pltpu.make_async_copy(moment, moment_out, sems.at[0]),
        pltpu.make_async_copy(weight, weight_out, sems.at[1]),
    ]
    for copy in copies:
        copy.start()
    for copy in copies:
        copy.wait()


def load(moment, weight):
    anywhere = pl.BlockSpec(memory_space=pl.ANY)
    return pl.pallas_call(
        load_body,
        in_specs=[anywhere] * 2,
        out_specs=[VMEM] * 2,
        out_shape=[pltpu.VMEM(moment.shape, F32), pltpu.VMEM(weight.shape, BF16)],
        scratch_shapes=[pltpu.SemaphoreType.DMA((2,))],
        compiler_params=params(1),
        name="load",
    )(moment, weight)


def finish_body(place, spread, total, moment, weight, mine, other, *refs):
    value_moment, value_weight = refs[:2]
    weight_out, moment_out, value_weight_out, value_moment_out = refs[2:]
    entry_count = 4 * (FF * D + D * KV)
    overall = jnp.sum(jnp.sum(spread[...], axis=0, keepdims=True), axis=1, keepdims=True)
    factor = jnp.minimum(1.0, math.sqrt(entry_count) / jnp.sqrt(overall + 1e-06))
    rows = pl.ds(pl.multiple_of(pl.program_id(0) * 224, 224), 224)
    following = MOMENTUM_DECAY * moment[0, rows, :] + factor * total[rows, :]
    moment_out[0] = following
    weight_out[0] = (weight[0, rows, :].astype(F32) - STEP_RATE * following).astype(BF16)

    @pl.when(pl.program_id(0) == 0)
    def _():
        for core, grad in ((place[3], mine), (1 - place[3], other)):
            columns = pl.ds(pl.multiple_of(core * 512, 512), 512)
            value_next = MOMENTUM_DECAY * value_moment[0, :, columns] + factor * grad[...].T
            value_moment_out[0, :, columns] = value_next
            value_weight_out[0, :, columns] = (
                value_weight[0, :, columns].astype(F32) - STEP_RATE * value_next
            ).astype(BF16)


def finish(*operands):
    block = pl.BlockSpec((1, 224, 1024), lambda i: (0, i, 0))
    small = pl.BlockSpec((1, 128, KV), lambda i: (0, 0, 0))
    return pl.pallas_call(
        finish_body,
        grid=(4,),
        in_specs=[SMEM] + [VMEM] * 8,
        out_specs=[block, block, small, small],
        out_shape=[
            like(1, 896, 1024),
            like(1, 896, 1024, dtype=F32),
            like(1, 128, KV),
            like(1, 128, KV, dtype=F32),
        ],
        compiler_params=params(16),
        name="finish",
    )(*operands)


def step(
    normed_inputs,
    value_cotangent,
    expert_hidden,
    expert_cotangent,
    slot_gate,
    slot_count,
    expert_weight,
    expert_moment,
    value_weight,
    value_moment,
):
    place = jnp.stack([lax.axis_index(axis) for axis in ("z", "xh", "xl", "c")])

    inputs_peer = flip(normed_inputs, "c", 2, 1)
    tokens_peer = flip(value_cotangent, "c", 2, 1)

    scaled = scale(place, slot_count, slot_gate, expert_cotangent)
    rows = {0: scaled[0]}
    for bits in (1, 2, 6, 3, 7, 4, 5):
        rows[bits] = flip(scaled[bits % 4], ROW, 8, bits)
    own_a = stack(rows[0], rows[1])
    own_h = stack(rows[2], rows[6], rows[3], rows[7])
    own_b = stack(rows[4], rows[5])

    own, pair, opposite, cross = value_product(
        place, normed_inputs, inputs_peer, value_cotangent, tokens_peer
    )
    opposite = flip(opposite, X, 4, 3)
    cross = flip(cross, X, 4, 3)
    pair = wide_sum(pair, opposite).astype(BF16)
    pair = flip(pair, X, 4, 1)
    terms = list(spread_rows(place, own, cross, pair))
    for bits in (2, 1, 3):
        terms[bits] = flip(terms[bits], "z", 4, bits)
    mine, other = halve(place, *terms)
    other = flip(other, "c", 2, 1)

    halves = arrange_hidden(place, expert_hidden)
    held = []
    for half in halves:
        core = flip(half, "c", 2, 1)
        paired = flip(half, X, 4, 1)
        both = flip(paired, "c", 2, 1)
        held.append([half, core, paired, both])

    ups = []
    downs = []
    for piece in (own_a, own_h, own_b):
        ups.append(shift(piece, "z", 1))
        downs.append(shift(piece, "z", -1))
    far_h = shift(ups[1], "z", 1)
    far_a = shift(downs[0], "z", -1)
    far_b = shift(downs[2], "z", -1)

    moment, weight = load(expert_moment, expert_weight)
    (total,) = contract(held[0], (0, 1), [(own_a, own_h, own_b), ups])
    (total,) = contract(held[1], (0,), [downs], total)
    total, slot = contract(held[1], (1,), [(far_a, far_h, far_b)], total, (mine, other))
    slots = lax.all_to_all(slot, ("section", "z", "xh", "xl", "c"), 0, 0, tiled=True)
    return finish(
        place, slots, total, moment, weight, mine, other, value_moment, value_weight
    )


def solution(mesh):
    finer = Mesh(
        mesh.devices.reshape(mesh.shape["section"], 4, 2, 2, 2),
        ("section", "z", "xh", "xl", "c"),
    )
    in_specs = (
        P("section", NARROW, None, WIDE, None),
        P("section", NARROW, None, WIDE, None),
        P("section", NARROW, None, None, WIDE),
        P("section", NARROW, None, WIDE, None),
        P("section", NARROW, None, WIDE),
        P("section", NARROW, None),
        P("section", WIDE, NARROW),
        P("section", WIDE, NARROW),
        P("section", WIDE_NARROW, None),
        P("section", WIDE_NARROW, None),
    )
    out_specs = (
        P("section", WIDE, NARROW),
        P("section", WIDE, NARROW),
        P("section", WIDE_NARROW, None),
        P("section", WIDE_NARROW, None),
    )
    return jax.shard_map(step, mesh=finer, in_specs=in_specs, out_specs=out_specs, check_vma=False)
```

```python
import math

import jax
import jax.numpy as jnp
from jax import lax
from jax.experimental import pallas as pl
from jax.experimental.pallas import tpu as pltpu
from jax.sharding import Mesh
from jax.sharding import PartitionSpec as P

D = 4096
FF = 7168
KV = 1024
WIDE = ("z", "xh")
NARROW = ("xl", "c")
ROW = ("xh", "xl", "c")
X = ("xh", "xl")
WIDE_NARROW = ("z", "xh", "xl", "c")

MOMENTUM_DECAY = 0.9
STEP_RATE = 0.01


def flip(value, axes, size, bits):
    return lax.ppermute(value, axes, [(i, i ^ bits) for i in range(size)])


def shift(value, axes, step):
    return lax.ppermute(value, axes, [(i, (i + step) % 4) for i in range(4)])


def wide_sum(*terms):
    total = terms[0].astype(jnp.float32)
    for term in terms[1:]:
        total = total + term.astype(jnp.float32)
    return total


F32 = jnp.float32
BF16 = jnp.bfloat16


def like(*shape, dtype=BF16):
    return jax.ShapeDtypeStruct(shape, dtype)


def params(mebibytes):
    return pltpu.CompilerParams(vmem_limit_bytes=mebibytes << 20)


SMEM = pl.BlockSpec(memory_space=pltpu.SMEM)
VMEM = pl.BlockSpec(memory_space=pltpu.VMEM)
ANY = pl.BlockSpec(memory_space=pl.ANY)


def scale_body(place, count, gate, cotangent, *outs):
    eye = lax.broadcasted_iota(jnp.int32, (32, 32), 0) == lax.broadcasted_iota(
        jnp.int32, (32, 32), 1
    )
    position = (place[0] * 2 + place[1]) * 32 + lax.broadcasted_iota(jnp.int32, (32, 1), 0)
    for m in range(4):
        row = gate[0, 0, m : m + 1, :].astype(F32)
        column = jnp.sum(jnp.where(eye, row, 0.0), axis=1, keepdims=True)
        coefficient = jnp.where(position < count[0, 0, m], column, 0.0)
        for bits in range(4):
            start = pl.multiple_of(((place[2] * 2 + place[3]) ^ bits) * 1024, 1024)
            piece = cotangent[0, 0, m, :, pl.ds(start, 1024)].astype(F32)
            outs[bits][m * 32 : m * 32 + 32, :] = (coefficient * piece).astype(BF16)


def scale(place, count, gate, cotangent):
    return pl.pallas_call(
        scale_body,
        in_specs=[SMEM, SMEM, VMEM, VMEM],
        out_specs=[VMEM] * 4,
        out_shape=[like(128, 1024)] * 4,
        compiler_params=params(8),
        name="scale",
    )(place, count, gate, cotangent)


def hidden_body(place, hidden, first, second):
    turned = hidden[0, 0].reshape(128, 896).T
    step = pl.program_id(0)

    @pl.when(step < 6)
    def _():
        first[...] = turned

    @pl.when(step >= 6)
    def _():
        second[...] = turned


def hidden_source(i, place):
    chunk = i // 2
    offset = jnp.where(chunk == 1, 3, jnp.where(chunk == 2, 1, jnp.where(chunk == 3, 2, 0)))
    source = (place[0] + offset) % 4
    return (0, 0, 0, source * 2 + (place[1] ^ (i % 2)), 0)


def arrange_hidden(place, hidden):
    return pl.pallas_call(
        hidden_body,
        grid_spec=pltpu.PrefetchScalarGridSpec(
            num_scalar_prefetch=1,
            grid=(8,),
            in_specs=[pl.BlockSpec((1, 1, 4, 32, 896), hidden_source)],
            out_specs=[
                pl.BlockSpec((896, 128), lambda i, place: (0, jnp.minimum(i, 5))),
                pl.BlockSpec((896, 128), lambda i, place: (0, jnp.maximum(i, 6) - 6)),
            ],
        ),
        out_shape=[like(896, 768), like(896, 256)],
        compiler_params=params(6),
        name="arrange_hidden",
    )(place, hidden)


def value_body(place, left_own, left_peer, right_own, right_peer, *refs):
    outs, turned = refs[:4], refs[4]

    @pl.when(pl.program_id(0) == 0)
    def _():
        half = pl.ds(pl.multiple_of(place[3] * 512, 512), 512)
        turned[:, :384] = right_own[0, 0, :, :, half].reshape(384, 512).T
        turned[:, 384:] = right_peer[0, 0, :, :, half].reshape(384, 512).T

    for bits in range(4):
        x = (place[1] * 2 + place[2]) ^ bits
        columns = pl.ds(pl.multiple_of(x * 256, 256), 256)
        left = jnp.concatenate(
            [ref[0, 0, :, :, columns].reshape(384, 256) for ref in (left_own, left_peer)]
        )
        outs[bits][0] = jnp.dot(turned[...], left, preferred_element_type=F32).astype(BF16)


def value_product(place, left_own, left_peer, right_own, right_peer):
    left = pl.BlockSpec((1, 1, 4, 96, 1024), lambda i, place: (0, 0, 0, 0, i))
    right = pl.BlockSpec((1, 1, 4, 96, KV), lambda i, place: (0, 0, 0, 0, 0))
    return pl.pallas_call(
        value_body,
        grid_spec=pltpu.PrefetchScalarGridSpec(
            num_scalar_prefetch=1,
            grid=(4,),
            in_specs=[left, left, right, right],
            out_specs=[pl.BlockSpec((1, 512, 256), lambda i, place: (i, 0, 0))] * 4,
            scratch_shapes=[pltpu.VMEM((512, 768), BF16)],
        ),
        out_shape=[like(4, 512, 256)] * 4,
        compiler_params=params(20),
        cost_estimate=pl.CostEstimate(
            flops=3221225472, bytes_accessed=12000000, transcendentals=0
        ),
        name="value_product",
    )(place, left_own, left_peer, right_own, right_peer)


def spread_body(place, own, first, second, *outs):
    total = own[0].astype(F32) + first[0].astype(F32) + second[0].astype(F32)
    for bits in range(4):

        @pl.when(pl.program_id(0) == bits)
        def _():
            outs[bits][...] = total.astype(BF16)


def spread_rows(place, own, first, second):
    block = pl.BlockSpec((1, 512, 256), lambda i, place: (place[0] ^ i, 0, 0))
    return pl.pallas_call(
        spread_body,
        grid_spec=pltpu.PrefetchScalarGridSpec(
            num_scalar_prefetch=1,
            grid=(4,),
            in_specs=[block] * 3,
            out_specs=[pl.BlockSpec((512, 256), lambda i, place: (0, 0))] * 4,
        ),
        out_shape=[like(512, 256)] * 4,
        compiler_params=params(8),
        name="spread_rows",
    )(place, own, first, second)


def halve_body(place, folded, *refs):
    terms, (mine, other, slot, total) = refs[:4], refs[4:]
    value = sum(term[...].astype(F32) for term in terms)
    total[...] = value
    mine[...] = total[:, pl.ds(pl.multiple_of(place[3] * 128, 128), 128)]
    other[...] = total[:, pl.ds(pl.multiple_of(128 - place[3] * 128, 128), 128)]
    squares = jnp.sum((value * value).reshape(64, 8, 256), axis=0)
    squares = folded[...] + squares[:, :128] + squares[:, 128:]
    slot[...] = jnp.broadcast_to(jnp.sum(squares, axis=0, keepdims=True), (128, 128))


def halve(place, folded, *terms):
    return pl.pallas_call(
        halve_body,
        in_specs=[SMEM] + [VMEM] * 5,
        out_specs=[VMEM] * 3,
        out_shape=[like(512, 128, dtype=F32)] * 2 + [like(128, 128, dtype=F32)],
        scratch_shapes=[pltpu.VMEM((512, 256), F32)],
        compiler_params=params(6),
        name="halve",
    )(place, folded, *terms)


def stack_body(*refs):
    for n, ref in enumerate(refs[:-1]):
        refs[-1][n * 128 : n * 128 + 128, :] = ref[...]


def stack(*pieces):
    return pl.pallas_call(
        stack_body,
        in_specs=[VMEM] * len(pieces),
        out_specs=VMEM,
        out_shape=like(128 * len(pieces), 1024),
        compiler_params=params(6),
        name="stack",
    )(*pieces)


def contract(hidden, places, rows, start=None, squares=False):
    count = len(places)
    width = 256

    def body(*refs):
        held = refs[: 4 * count]
        pieces = refs[4 * count : 7 * count]
        rest = list(refs[7 * count :])
        columns = pl.ds(pl.multiple_of(pl.program_id(0) * width, width), width)
        left = jnp.concatenate([h[...] for h in held], axis=1)
        right = []
        for n in range(count):
            a, p, q = pieces[3 * n : 3 * n + 3]
            for m, piece in enumerate((a, a, p, p)):
                near = m % 2 * 128
                right += [piece[near : near + 128], q[m * 128 : m * 128 + 128]]
        total = jnp.dot(left, jnp.concatenate(right), preferred_element_type=F32)
        if start is not None:
            total = total + rest.pop(0)[:, columns]
        rest[0][:, columns] = total
        if squares:
            folded = jnp.sum((total * total).reshape(112, 8, width), axis=0)
            folded = folded[:, :128] + folded[:, 128:]

            @pl.when(pl.program_id(0) == 0)
            def _():
                rest[1][...] = folded

            @pl.when(pl.program_id(0) > 0)
            def _():
                rest[1][...] = rest[1][...] + folded

    def held(k):
        return pl.BlockSpec((896, 256), lambda i: (0, k))

    def piece(rows):
        return pl.BlockSpec((rows, width), lambda i: (0, i))

    extra = [] if start is None else [start]
    out_shape = [pltpu.VMEM((896, 1024), F32)]
    if squares:
        out_shape.append(like(8, 128, dtype=F32))
    return pl.pallas_call(
        body,
        grid=(1024 // width,),
        in_specs=[held(k) for k in places for _ in range(4)]
        + [piece(256), piece(256), piece(512)] * count
        + [VMEM] * len(extra),
        out_specs=[VMEM] * len(out_shape),
        out_shape=out_shape,
        cost_estimate=pl.CostEstimate(
            flops=count * 1879048192, bytes_accessed=count * 4000000, transcendentals=0
        ),
        compiler_params=params(28),
        name="contract",
    )(*[h for _ in places for h in hidden], *[p for three in rows for p in three], *extra)


def load_body(*refs):
    sems = refs[8]
    copies = [pltpu.make_async_copy(refs[n], refs[n + 4], sems.at[n]) for n in range(4)]
    for copy in copies:
        copy.start()
    for copy in copies:
        copy.wait()


def load(*arrays):
    return pl.pallas_call(
        load_body,
        in_specs=[ANY] * 4,
        out_specs=[VMEM] * 4,
        out_shape=[pltpu.VMEM(a.shape, a.dtype) for a in arrays],
        scratch_shapes=[pltpu.SemaphoreType.DMA((4,))],
        compiler_params=params(1),
        name="load",
    )(*arrays)


def finish_body(place, spread, total, moment, weight, mine, other, *refs):
    value_moment, value_weight = refs[:2]
    outs, held, sems = refs[2:6], refs[6:10], refs[10]
    entry_count = 4 * (FF * D + D * KV)
    overall = jnp.sum(jnp.sum(spread[...], axis=0, keepdims=True), axis=1, keepdims=True)
    factor = jnp.minimum(1.0, math.sqrt(entry_count) / jnp.sqrt(overall + 1e-06))
    copies = []

    def send(n, m, rows):
        copy = pltpu.make_async_copy(held[n].at[:, rows], outs[n].at[:, rows], sems.at[n, m])
        copy.start()
        copies.append(copy)

    for m in range(8):
        rows = slice(m * 112, m * 112 + 112)
        following = MOMENTUM_DECAY * moment[0, rows] + factor * total[rows]
        held[1][0, rows] = following
        send(1, m, pl.ds(m * 112, 112))
        held[0][0, rows] = (weight[0, rows].astype(F32) - STEP_RATE * following).astype(BF16)
        send(0, m, pl.ds(m * 112, 112))
    for core, grad in ((place[3], mine), (1 - place[3], other)):
        columns = pl.ds(pl.multiple_of(core * 512, 512), 512)
        value_next = MOMENTUM_DECAY * value_moment[0, :, columns] + factor * grad[...].T
        held[3][0, :, columns] = value_next
        held[2][0, :, columns] = (
            value_weight[0, :, columns].astype(F32) - STEP_RATE * value_next
        ).astype(BF16)
    send(2, 0, pl.ds(0, 128))
    send(3, 0, pl.ds(0, 128))
    for copy in copies:
        copy.wait()


def finish(*operands):
    shapes = [((1, 896, 1024), BF16), ((1, 896, 1024), F32), ((1, 128, KV), BF16)]
    shapes.append(((1, 128, KV), F32))
    return pl.pallas_call(
        finish_body,
        in_specs=[SMEM] + [VMEM] * 8,
        out_specs=[ANY] * 4,
        out_shape=[like(*shape, dtype=dtype) for shape, dtype in shapes],
        scratch_shapes=[pltpu.VMEM(shape, dtype) for shape, dtype in shapes]
        + [pltpu.SemaphoreType.DMA((4, 8))],
        compiler_params=params(16),
        name="finish",
    )(*operands)


def step(
    normed_inputs,
    value_cotangent,
    expert_hidden,
    expert_cotangent,
    slot_gate,
    slot_count,
    expert_weight,
    expert_moment,
    value_weight,
    value_moment,
):
    place = jnp.stack([lax.axis_index(axis) for axis in ("z", "xh", "xl", "c")])

    inputs_peer = flip(normed_inputs, "c", 2, 1)
    tokens_peer = flip(value_cotangent, "c", 2, 1)

    scaled = scale(place, slot_count, slot_gate, expert_cotangent)
    rows = {0: scaled[0]}
    for bits in (1, 2, 6, 3, 7, 4, 5):
        rows[bits] = flip(scaled[bits % 4], ROW, 8, bits)
    own_a = stack(rows[0], rows[1])
    own_p = stack(rows[2], rows[3])
    own_q = stack(rows[4], rows[5], rows[6], rows[7])

    own, pair, opposite, cross = value_product(
        place, normed_inputs, inputs_peer, value_cotangent, tokens_peer
    )
    opposite = flip(opposite, X, 4, 3)
    cross = flip(cross, X, 4, 3)
    pair = wide_sum(pair, opposite).astype(BF16)
    pair = flip(pair, X, 4, 1)
    terms = list(spread_rows(place, own, cross, pair))
    for bits in (2, 1, 3):
        terms[bits] = flip(terms[bits], "z", 4, bits)
    halves = arrange_hidden(place, expert_hidden)
    held = []
    for half in halves:
        core = flip(half, "c", 2, 1)
        paired = flip(half, X, 4, 1)
        both = flip(paired, "c", 2, 1)
        held.append([half, core, paired, both])

    ups = []
    downs = []
    for piece in (own_a, own_p, own_q):
        ups.append(shift(piece, "z", 1))
        downs.append(shift(piece, "z", -1))
    far_a = shift(downs[0], "z", -1)
    far_p = shift(downs[1], "z", -1)
    far_q = shift(ups[2], "z", 1)

    loaded = load(expert_moment, expert_weight, value_moment, value_weight)
    (total,) = contract(held[0], (0, 1), [(own_a, own_p, own_q), ups])
    (total,) = contract(held[0], (2,), [downs], total)
    total, folded = contract(held[1], (0,), [(far_a, far_p, far_q)], total, True)
    mine, other, slot = halve(place, folded, *terms)
    other = flip(other, "c", 2, 1)
    slots = lax.all_to_all(slot, ("section", "z", "xh", "xl", "c"), 0, 0, tiled=True)
    return finish(place, slots, total, *loaded[:2], mine, other, *loaded[2:])


def solution(mesh):
    finer = Mesh(
        mesh.devices.reshape(mesh.shape["section"], 4, 2, 2, 2),
        ("section", "z", "xh", "xl", "c"),
    )
    in_specs = (
        P("section", NARROW, None, WIDE, None),
        P("section", NARROW, None, WIDE, None),
        P("section", NARROW, None, None, WIDE),
        P("section", NARROW, None, WIDE, None),
        P("section", NARROW, None, WIDE),
        P("section", NARROW, None),
        P("section", WIDE, NARROW),
        P("section", WIDE, NARROW),
        P("section", WIDE_NARROW, None),
        P("section", WIDE_NARROW, None),
    )
    out_specs = (
        P("section", WIDE, NARROW),
        P("section", WIDE, NARROW),
        P("section", WIDE_NARROW, None),
        P("section", WIDE_NARROW, None),
    )
    return jax.shard_map(step, mesh=finer, in_specs=in_specs, out_specs=out_specs, check_vma=False)
```
